256 devices in a mesh: kpt: 4 (over y_lo, core), row: 8 (over z), col: 8 (over y_hi, x).
Axes of the slice: x: 4, y: 4 (y_hi: 2, y_lo: 2; y = y_hi * 2 + y_lo), z: 8, core: 2. Of those that a mesh axis runs over, the one named last changes fastest.
Arguments:
- a_matrix: bfloat16 [8, 4096, 4096], P('kpt', 'row', 'col'), parts along dimension 0, may hold values from -6 to 6
- b_matrix: bfloat16 [8, 4096, 4096], P('kpt', 'row', 'col'), parts along dimension 0, may hold values from -0.09375 to 0.09375
- a_level: int32 [128, 32], P('kpt'), parts along dimension 0, may hold values from 0 to 4, as said below
- b_level: int32 [128, 32], P('kpt'), parts along dimension 0, may hold values from 0 to 4, as said below
- limit: int32 [128, 32], P(('kpt', 'row'), 'col'), parts along dimension 0, may hold values from 3 to 8
Outputs:
- product: bfloat16 [8, 4096, 4096], P('kpt', 'row', 'col'), parts along dimension 0
- kept_count: int32 [128, 32], P(('kpt', 'row'), 'col'), parts along dimension 0
- kept_total: int32 [4], P('kpt'), parts along dimension 0
The draws below stay inside these ranges and needn't reach their ends.
There are 4 independent parts, one for each index of `kpt`. The reference program is written for one: setup_inputs(seed, part) draws one part's arguments, and reference() takes and returns one part's arrays. A program takes and returns all parts, laid end to end along the dimension named above; each array names one. Nothing has to cross between parts.
Inputs may be any that keep to these rules, and one draw needn't show every extreme that they name: Each block's level is 0 (empty) or its norm exponent 1 to 4; the share of occupied blocks rises from some a sixth in the first block row of a_level (block column of b_level) to some six in seven in the last. `b_level`: as for a_level, with the share rising along block columns.
All inputs are finite; a program needn't handle non-finite values.
Results may differ from the reference program's by a relative error of at most 0.001.
Values may be sent and summed in bfloat16 or wider, within the bound.
A program may use at most 128 MiB of HBM per device.

```python
import jax
import jax.numpy as jnp
from jax import lax

ORDER = 4096
BLK = 128
NBLK = 32


def skewed_levels(key, along_rows):
    first, second = jax.random.split(jax.random.fold_in(key, 71))
    chance = jax.random.randint(first, (NBLK, NBLK), 0, 100)
    level = jax.random.randint(second, (NBLK, NBLK), 1, 5)
    steps = jnp.arange(NBLK, dtype=jnp.int32)
    percent = 15 + 70 * steps // (NBLK - 1)
    bound = percent[:, None] if along_rows else percent[None, :]
    return jnp.where(chance < bound, level, 0).astype(jnp.int32)


def draw_a_level(key, part):
    return skewed_levels(jax.random.fold_in(key, 3), True)


def draw_b_level(key, part):
    return skewed_levels(jax.random.fold_in(key, 5), False)


def touch_ends(entries, rng, smallest, largest):
    longest = entries.shape.index(max(entries.shape))
    spots = []
    for shift in (0, 1):
        where = [jax.random.randint(jax.random.fold_in(rng, axis), (), 0, length) for axis, length in enumerate(entries.shape)]
        where[longest] = (where[longest] + shift) % entries.shape[longest]
        spots.append(tuple(where))
    return entries.at[spots[0]].set(smallest).at[spots[1]].set(largest)


def level_of(rng, dims, cuts, least, top_value):
    level = 1.0
    for axis_at, parts in cuts:
        heights = jax.random.uniform(jax.random.fold_in(jax.random.fold_in(rng, 6), axis_at), (parts,), jnp.float32, least / len(cuts), top_value / len(cuts))
        level = level * jnp.repeat(jnp.exp(heights), dims[axis_at] // parts).reshape((-1,) + (1,) * (len(dims) - 1 - axis_at))
    return level


def normal_values(key, dims, spread, most, cuts=(), kind=jnp.bfloat16):
    values = jax.random.normal(key, dims, jnp.float32) * spread
    if len(cuts) > 0:
        values = level_of(key, dims, cuts, -0.22, 0.18) * values
    return jnp.clip(values, min=-most, max=most).astype(kind)


def setup_inputs(seed: int = 0, part: int = 0) -> dict:
    key_of = jax.random.split(jax.random.key(seed), 6)
    part_splits = jax.random.split(jax.random.fold_in(key_of[5], part), 6)
    a_matrix = normal_values(part_splits[0], (2, ORDER, ORDER), 1.0, 6.0, ((1, 8), (2, 8)))
    b_matrix = normal_values(part_splits[1], (2, ORDER, ORDER), ORDER ** -0.5, 0.09375, ((1, 8), (2, 8)))
    a_level = draw_a_level(jax.random.fold_in(jax.random.fold_in(key_of[5], part), 71), part)
    b_level = draw_b_level(jax.random.fold_in(jax.random.fold_in(key_of[5], part), 71), part)
    limit = touch_ends(jax.random.randint(part_splits[4], (NBLK, NBLK), 3, 9), jax.random.fold_in(part_splits[4], 1), 3, 8).astype(jnp.int32)
    return {"a_matrix": a_matrix, "b_matrix": b_matrix, "a_level": a_level, "b_level": b_level, "limit": limit}


def level_scale(levels):
    power = jnp.power(jnp.float32(2.0), (1 - levels).astype(jnp.float32))
    return jnp.where(levels > 0, power, jnp.float32(0.0))


def spread_blocks(small):
    return jnp.repeat(jnp.repeat(small, BLK, axis=0), BLK, axis=1)


def reference(a_matrix, b_matrix, a_level, b_level, limit):
    a_eff = a_matrix * spread_blocks(level_scale(a_level)).astype(jnp.bfloat16)[None]
    b_eff = b_matrix * spread_blocks(level_scale(b_level)).astype(jnp.bfloat16)[None]
    keep = (a_level[:, :, None] > 0) & (b_level[None, :, :] > 0) & (a_level[:, :, None] + b_level[None, :, :] <= limit[:, None, :])
    kept_count = jnp.sum(keep.astype(jnp.int32), axis=1).astype(jnp.int32)
    kept_total = jnp.sum(kept_count).reshape(1).astype(jnp.int32)

    def one_column(index):
        mask = spread_blocks(lax.dynamic_index_in_dim(keep, index, 2, keepdims=False))
        masked = jnp.where(mask[None], a_eff, jnp.zeros((), jnp.bfloat16))
        column = lax.dynamic_slice_in_dim(b_eff, (index * BLK).astype(jnp.int32), BLK, 2)
        real_real = jnp.dot(masked[0], column[0], preferred_element_type=jnp.float32)
        imag_imag = jnp.dot(masked[1], column[1], preferred_element_type=jnp.float32)
        real_imag = jnp.dot(masked[0], column[1], preferred_element_type=jnp.float32)
        imag_real = jnp.dot(masked[1], column[0], preferred_element_type=jnp.float32)
        return jnp.stack([real_real - imag_imag, real_imag + imag_real])

    columns = lax.map(one_column, jnp.arange(NBLK, dtype=jnp.int32))
    product = jnp.transpose(columns, (1, 2, 0, 3)).reshape(2, ORDER, ORDER).astype(jnp.bfloat16)
    return product, kept_count, kept_total
```

```python
import functools

import jax
import jax.numpy as jnp
from jax import lax
from jax.experimental import pallas as pl
from jax.experimental.pallas import tpu as pltpu
from jax.sharding import PartitionSpec as P

BLK = 128
Z = 8
X = 4
PIECES = 4
Z_STREAM = 14
X_STREAM = 12
MESH = pl.DeviceIdType.MESH


def piece(ref, slot, q):
    return ref.at[slot, :, pl.ds(pl.multiple_of(q * BLK, BLK), BLK), :]


def kernel(
    a_lev, b_lev, lim, a_hbm, b_hbm,
    out, cnt_out, tot_out,
    a_buf, b_buf, acc, scale, own_cnt, row_cnt, sum_cnt, col_cnt,
    in_sem, zr_send, zr_recv, zl_send, zl_recv,
    xr_send, xr_recv, xl_send, xl_recv, y_send, y_recv,
    rc_send, rc_recv, cc_send, cc_recv,
):
    z = lax.axis_index("row")
    c = lax.axis_index("col")
    x = c % X
    yh = c // X
    z_right, z_left = (z + 1) % Z, (z + Z - 1) % Z

    def col_at(dx, dy):
        return ((yh + dy) % 2) * X + (x + dx + X) % X

    x_right, x_left, y_far = col_at(1, 0), col_at(-1, 0), col_at(0, 1)

    a_in = pltpu.make_async_copy(a_hbm, a_buf.at[c], in_sem.at[0])
    b_in = pltpu.make_async_copy(b_hbm, b_buf.at[z], in_sem.at[1])
    b_in.start()
    a_in.start()

    barrier = pltpu.get_barrier_semaphore()
    for there in (z_right, z_left):
        pl.semaphore_signal(barrier, inc=1, device_id={"row": there}, device_id_type=MESH)
    for there in (x_right, x_left, y_far):
        pl.semaphore_signal(barrier, inc=1, device_id={"col": there}, device_id_type=MESH)
    pl.semaphore_wait(barrier, 5)
    b_in.wait()
    a_in.wait()

    def z_copy(right, t, sending):
        whole = t < 12
        far = jnp.where(whole, t // PIECES, 3)
        if right:
            q = jnp.where(whole, t % PIECES, t - 12)
            origin = (z - far - (0 if sending else 1) + 2 * Z) % Z
            sems = (zr_send.at[t], zr_recv.at[t])
            there = z_right
        else:
            q = jnp.where(whole, t % PIECES, t - 10)
            origin = (z + far + (0 if sending else 1)) % Z
            sems = (zl_send.at[t], zl_recv.at[t])
            there = z_left
        part = piece(b_buf, origin, q)
        return pltpu.make_async_remote_copy(
            part, part, *sems, device_id={"row": there}, device_id_type=MESH
        )

    def x_copy(right, u, sending):
        second = u >= 6
        v = jnp.where(second, u - 6, u)
        relayed = v >= 4
        dx = jnp.where(relayed, 1, 0) + (0 if sending else 1)
        dy = jnp.where(second, 1, 0)
        if right:
            q = jnp.where(relayed, v - 4, v)
            sems = (xr_send.at[u], xr_recv.at[u])
            origin, there = col_at(-dx, dy), x_right
        else:
            q = jnp.where(relayed, v - 2, v)
            sems = (xl_send.at[u], xl_recv.at[u])
            origin, there = col_at(dx, dy), x_left
        part = piece(a_buf, origin, q)
        return pltpu.make_async_remote_copy(
            part, part, *sems, device_id={"col": there}, device_id_type=MESH
        )

    def y_copy(v, sending):
        part = piece(a_buf, c if sending else y_far, v)
        return pltpu.make_async_remote_copy(
            part, part, y_send.at[v], y_recv.at[v], device_id={"col": y_far}, device_id_type=MESH
        )

    def count_to_row(d):
        return pltpu.make_async_remote_copy(
            own_cnt, row_cnt.at[d - 1], rc_send.at[d - 1], rc_recv.at[d - 1],
            device_id={"col": (c + d) % 8}, device_id_type=MESH,
        )

    def count_to_col(d):
        return pltpu.make_async_remote_copy(
            sum_cnt, col_cnt.at[d - 1], cc_send.at[d - 1], cc_recv.at[d - 1],
            device_id={"row": (z + d) % Z}, device_id_type=MESH,
        )

    def z_send(t):
        z_copy(True, t, True).start()
        z_copy(False, t, True).start()

    def x_send(u):
        x_copy(True, u, True).start()
        x_copy(False, u, True).start()

    z_send(0)
    x_send(0)
    y_copy(0, True).start()
    z_send(1)
    x_send(1)
    for v in range(1, PIECES):
        y_copy(v, True).start()

    def tabulate(k, counts):
        new = []
        for i in range(4):
            a = a_lev[4 * z + i, k]
            for j in range(4):
                b = b_lev[k, 4 * c + j]
                keep = (a > 0) & (b > 0) & (a + b <= lim[i, j])
                near = jnp.where(a + b >= 6, 4, a + b - 2)
                power = jnp.where(
                    a + b <= 4,
                    jnp.where(a + b <= 2, 1.0, jnp.where(a + b <= 3, 0.5, 0.25)),
                    jnp.where(
                        a + b <= 6,
                        jnp.where(a + b <= 5, 0.125, 0.0625),
                        jnp.where(a + b <= 7, 0.03125, 0.015625),
                    ),
                )
                scale[k, i * 4 + j] = jnp.where(keep, power, 0.0).astype(jnp.float32)
                new.append(counts[i * 4 + j] + jnp.where(keep, 1, 0))
        return tuple(new)

    counts = lax.fori_loop(0, 32, tabulate, (jnp.int32(0),) * 16)
    total = jnp.int32(0)
    for i in range(4):
        for j in range(4):
            cnt_out[i, j] = counts[i * 4 + j]
            total = total + counts[i * 4 + j]
    own_cnt[...] = jnp.full(own_cnt.shape, total, jnp.int32)
    acc[...] = jnp.zeros_like(acc)

    def multiply(m, q):
        k = 4 * m + q
        lane = pl.ds(pl.multiple_of(q * BLK, BLK), BLK)

        def one_column(j, _):
            cols = pl.ds(pl.multiple_of(j * BLK, BLK), BLK)
            b_re = b_buf[m, 0, lane, cols]
            b_im = b_buf[m, 1, lane, cols]
            right = jnp.concatenate(
                [jnp.concatenate([b_re, b_im], 1), jnp.concatenate([-b_im, b_re], 1)], 0
            )
            lefts = []
            for i in range(4):
                rows = pl.ds(i * BLK, BLK)
                by = scale[k, i * 4 + j].astype(jnp.bfloat16)
                lefts.append(
                    jnp.concatenate([a_buf[m, 0, rows, lane], a_buf[m, 1, rows, lane]], 1) * by
                )
            left = jnp.concatenate(lefts, 0)
            acc[j] += jnp.dot(left, right, preferred_element_type=jnp.float32)
            return 0

        lax.fori_loop(0, 4, one_column, 0)

    def a_slot_time(m):
        dx = (m % X - x + X) % X
        dy = jnp.where(m // X == yh, 0, 1)
        same = jnp.where(dx == 0, 0, jnp.where(dx == 2, 5, 3))
        other = jnp.where(dx == 0, 9, jnp.where(dx == 2, 13, 11))
        return jnp.where(dy == 0, same, other)

    def b_slot_time(m, q):
        d = (m - z + Z) % Z
        near = jnp.minimum(d, Z - d)
        return jnp.where(near == 0, 0, jnp.where(near == 4, 12 + q % 2, 4 * near - 4 + q))

    def x_step(slot):
        for u, at in enumerate((0, 1, 2, 3, 4, 5, 7, 8, 9, 11, 12, 13)):
            @pl.when(slot == at)
            def _():
                x_copy(True, u, False).wait_recv()
                x_copy(False, u, False).wait_recv()

        for v, at in enumerate((4, 6, 7, 9)):
            @pl.when(slot == at)
            def _():
                y_copy(v, False).wait_recv()

        for u, at in ((2, 0), (3, 1), (4, 2), (5, 3), (6, 4), (7, 6), (8, 7), (9, 9), (10, 9), (11, 11)):
            @pl.when(slot == at)
            def _():
                x_send(jnp.int32(u))

    def slot_body(slot, _):
        z_copy(True, slot, False).wait_recv()
        z_copy(False, slot, False).wait_recv()

        @pl.when(slot < Z_STREAM - 2)
        def _():
            z_send(slot + 2)

        x_step(slot)

        @pl.when(slot == 5)
        def _():
            for d in range(1, 8):
                count_to_row(d).start()

        @pl.when(slot == 8)
        def _():
            for d in range(1, 8):
                count_to_row(d).wait_recv()
            sum_cnt[...] = own_cnt[...] + jnp.sum(row_cnt[...], axis=0)

        @pl.when(slot == 9)
        def _():
            for d in range(1, 8):
                count_to_col(d).start()

        @pl.when(slot == 12)
        def _():
            for d in range(1, 8):
                count_to_col(d).wait_recv()
            everyone = sum_cnt[...] + jnp.sum(col_cnt[...], axis=0)
            tot_out[0] = everyone[0, 0]

        def one_source(m, _):
            a_at = a_slot_time(m)

            def one_piece(q, _):
                @pl.when(jnp.maximum(a_at, b_slot_time(m, q)) == slot)
                def _():
                    multiply(m, q)

                return 0

            @pl.when(a_at <= slot)
            def _():
                lax.fori_loop(0, PIECES, one_piece, 0)

            return 0

        lax.fori_loop(0, Z, one_source, 0)
        return 0

    lax.fori_loop(0, Z_STREAM, slot_body, 0)

    for j in range(4):
        for p in range(2):
            out[p, :, j * BLK : (j + 1) * BLK] = acc[j, :, p * BLK : (p + 1) * BLK].astype(
                jnp.bfloat16
            )

    def z_done(t, _):
        z_copy(True, t, True).wait_send()
        z_copy(False, t, True).wait_send()
        return 0

    def x_done(u, _):
        x_copy(True, u, True).wait_send()
        x_copy(False, u, True).wait_send()
        return 0

    def y_done(v, _):
        y_copy(v, True).wait_send()
        return 0

    lax.fori_loop(0, Z_STREAM, z_done, 0)
    lax.fori_loop(0, X_STREAM, x_done, 0)
    lax.fori_loop(0, PIECES, y_done, 0)
    for d in range(1, 8):
        count_to_row(d).wait_send()
        count_to_col(d).wait_send()


def shards(a_matrix, b_matrix, a_level, b_level, limit):
    parts, rows, columns = a_matrix.shape
    dma = pltpu.SemaphoreType.DMA
    smem = pl.BlockSpec(memory_space=pltpu.SMEM)
    hbm = pl.BlockSpec(memory_space=pl.ANY)
    return pl.pallas_call(
        kernel,
        out_shape=(
            jax.ShapeDtypeStruct((parts, rows, columns), jnp.bfloat16),
            jax.ShapeDtypeStruct((4, 4), jnp.int32),
            jax.ShapeDtypeStruct((1,), jnp.int32),
        ),
        in_specs=[smem, smem, smem, hbm, hbm],
        out_specs=(pl.BlockSpec(memory_space=pltpu.VMEM), smem, smem),
        scratch_shapes=[
            pltpu.VMEM((8, parts, rows, columns), jnp.bfloat16),
            pltpu.VMEM((Z, parts, rows, columns), jnp.bfloat16),
            pltpu.VMEM((4, rows, 2 * BLK), jnp.float32),
            pltpu.SMEM((32, 16), jnp.float32),
            pltpu.VMEM((8, BLK), jnp.int32),
            pltpu.VMEM((7, 8, BLK), jnp.int32),
            pltpu.VMEM((8, BLK), jnp.int32),
            pltpu.VMEM((7, 8, BLK), jnp.int32),
            dma((2,)),
            dma((Z_STREAM,)), dma((Z_STREAM,)), dma((Z_STREAM,)), dma((Z_STREAM,)),
            dma((X_STREAM,)), dma((X_STREAM,)), dma((X_STREAM,)), dma((X_STREAM,)),
            dma((PIECES,)), dma((PIECES,)),
            dma((7,)), dma((7,)), dma((7,)), dma((7,)),
        ],
        compiler_params=pltpu.CompilerParams(
            collective_id=0, has_side_effects=True, vmem_limit_bytes=40 * 1024 * 1024
        ),
        cost_estimate=pl.CostEstimate(
            flops=8 * rows * 4096 * columns, bytes_accessed=6 << 20, transcendentals=0
        ),
    )(a_level, b_level, limit, a_matrix, b_matrix)


def solution(mesh):
    placed = (
        P("kpt", "row", "col"),
        P("kpt", "row", "col"),
        P("kpt", None),
        P("kpt", None),
        P(("kpt", "row"), "col"),
    )
    return jax.shard_map(
        shards,
        mesh=mesh,
        in_specs=placed,
        out_specs=(P("kpt", "row", "col"), P(("kpt", "row"), "col"), P("kpt")),
        check_vma=False,
    )
```

```python
import functools

import jax
import jax.numpy as jnp
from jax import lax
from jax.experimental import pallas as pl
from jax.experimental.pallas import tpu as pltpu
from jax.sharding import PartitionSpec as P

BLK = 128
Z = 8
X = 4
PIECES = 4
Z_STREAM = 14
X_STREAM = 12
MESH = pl.DeviceIdType.MESH


def piece(ref, slot, q):
    return ref.at[slot, :, pl.ds(pl.multiple_of(q * BLK, BLK), BLK), :]


def kernel(
    a_lev_hbm, b_lev_hbm, lim_hbm, a_hbm, b_hbm,
    acc, cnt_out, tot_out,
    a_lev, b_lev, lim, a_buf, b_buf, scale, own_cnt, row_cnt, sum_cnt, col_cnt,
    lev_sem, in_sem, zr_send, zr_recv, zl_send, zl_recv,
    xr_send, xr_recv, xl_send, xl_recv, y_send, y_recv,
    rc_send, rc_recv, cc_send, cc_recv,
):
    z = lax.axis_index("row")
    c = lax.axis_index("col")
    x = c % X
    yh = c // X
    z_right, z_left = (z + 1) % Z, (z + Z - 1) % Z

    def col_at(dx, dy):
        return ((yh + dy) % 2) * X + (x + dx + X) % X

    x_right, x_left, y_far = col_at(1, 0), col_at(-1, 0), col_at(0, 1)

    a_in = pltpu.make_async_copy(a_hbm, a_buf.at[c], in_sem.at[0])
    b_in = pltpu.make_async_copy(b_hbm, b_buf.at[z], in_sem.at[1])
    b_in.start()
    a_in.start()
    levels_in = [
        pltpu.make_async_copy(there, here, lev_sem.at[n])
        for n, (there, here) in enumerate(
            ((a_lev_hbm, a_lev), (b_lev_hbm, b_lev), (lim_hbm, lim))
        )
    ]
    for copy in levels_in:
        copy.start()

    barrier = pltpu.get_barrier_semaphore()
    for there in (z_right, z_left):
        pl.semaphore_signal(barrier, inc=1, device_id={"row": there}, device_id_type=MESH)
    for there in (x_right, x_left, y_far):
        pl.semaphore_signal(barrier, inc=1, device_id={"col": there}, device_id_type=MESH)
    pl.semaphore_wait(barrier, 5)
    b_in.wait()
    a_in.wait()

    def z_copy(right, t, sending):
        whole = t < 12
        far = jnp.where(whole, t // PIECES, 3)
        if right:
            q = jnp.where(whole, t % PIECES, t - 12)
            origin = (z - far - (0 if sending else 1) + 2 * Z) % Z
            sems = (zr_send.at[t], zr_recv.at[t])
            there = z_right
        else:
            q = jnp.where(whole, t % PIECES, t - 10)
            origin = (z + far + (0 if sending else 1)) % Z
            sems = (zl_send.at[t], zl_recv.at[t])
            there = z_left
        part = piece(b_buf, origin, q)
        return pltpu.make_async_remote_copy(
            part, part, *sems, device_id={"row": there}, device_id_type=MESH
        )

    def x_copy(right, u, sending):
        second = u >= 6
        v = jnp.where(second, u - 6, u)
        relayed = v >= 4
        dx = jnp.where(relayed, 1, 0) + (0 if sending else 1)
        dy = jnp.where(second, 1, 0)
        if right:
            q = jnp.where(relayed, v - 4, v)
            sems = (xr_send.at[u], xr_recv.at[u])
            origin, there = col_at(-dx, dy), x_right
        else:
            q = jnp.where(relayed, v - 2, v)
            sems = (xl_send.at[u], xl_recv.at[u])
            origin, there = col_at(dx, dy), x_left
        part = piece(a_buf, origin, q)
        return pltpu.make_async_remote_copy(
            part, part, *sems, device_id={"col": there}, device_id_type=MESH
        )

    def y_copy(v, sending):
        part = piece(a_buf, c if sending else y_far, v)
        return pltpu.make_async_remote_copy(
            part, part, y_send.at[v], y_recv.at[v], device_id={"col": y_far}, device_id_type=MESH
        )

    def count_to_row(d):
        return pltpu.make_async_remote_copy(
            own_cnt, row_cnt.at[d - 1], rc_send.at[d - 1], rc_recv.at[d - 1],
            device_id={"col": (c + d) % 8}, device_id_type=MESH,
        )

    def count_to_col(d):
        return pltpu.make_async_remote_copy(
            sum_cnt, col_cnt.at[d - 1], cc_send.at[d - 1], cc_recv.at[d - 1],
            device_id={"row": (z + d) % Z}, device_id_type=MESH,
        )

    def z_send(t):
        z_copy(True, t, True).start()
        z_copy(False, t, True).start()

    def x_send(u):
        x_copy(True, u, True).start()
        x_copy(False, u, True).start()

    z_send(0)
    x_send(0)
    y_copy(0, True).start()
    z_send(1)
    x_send(1)
    for v in range(1, PIECES):
        y_copy(v, True).start()

    def tabulate(k, counts):
        new = []
        for i in range(4):
            a = a_lev[4 * z + i, k]
            for j in range(4):
                b = b_lev[k, 4 * c + j]
                keep = (a > 0) & (b > 0) & (a + b <= lim[i, j])
                power = jnp.where(
                    a + b <= 4,
                    jnp.where(a + b <= 2, 1.0, jnp.where(a + b <= 3, 0.5, 0.25)),
                    jnp.where(
                        a + b <= 6,
                        jnp.where(a + b <= 5, 0.125, 0.0625),
                        jnp.where(a + b <= 7, 0.03125, 0.015625),
                    ),
                )
                scale[k, i * 4 + j] = jnp.where(keep, power, 0.0).astype(jnp.float32)
                new.append(counts[i * 4 + j] + jnp.where(keep, 1, 0))
        return tuple(new)

    for copy in levels_in:
        copy.wait()
    counts = lax.fori_loop(0, 32, tabulate, (jnp.int32(0),) * 16)
    total = jnp.int32(0)
    for i in range(4):
        for j in range(4):
            cnt_out[i, j] = counts[i * 4 + j]
            total = total + counts[i * 4 + j]
    own_cnt[...] = jnp.full(own_cnt.shape, total, jnp.int32)
    acc[...] = jnp.zeros_like(acc)

    def multiply(m, q):
        k = 4 * m + q
        lane = pl.ds(pl.multiple_of(q * BLK, BLK), BLK)

        def one_column(j):
            cols = pl.ds(j * BLK, BLK)
            b_re = b_buf[m, 0, lane, cols]
            b_im = b_buf[m, 1, lane, cols]
            right = jnp.concatenate(
                [jnp.concatenate([b_re, b_im], 1), jnp.concatenate([-b_im, b_re], 1)], 0
            )
            lefts = []
            for i in range(4):
                rows = pl.ds(i * BLK, BLK)
                by = scale[k, i * 4 + j].astype(jnp.bfloat16)
                lefts.append(
                    jnp.concatenate([a_buf[m, 0, rows, lane], a_buf[m, 1, rows, lane]], 1) * by
                )
            left = jnp.concatenate(lefts, 0)
            both = jnp.dot(left, right, preferred_element_type=jnp.float32)
            acc[0, :, cols] += both[:, :BLK]
            acc[1, :, cols] += both[:, BLK:]

        for j in range(4):
            one_column(j)

    def a_slot_time(m):
        dx = (m % X - x + X) % X
        dy = jnp.where(m // X == yh, 0, 1)
        same = jnp.where(dx == 0, 0, jnp.where(dx == 2, 5, 3))
        other = jnp.where(dx == 0, 8, jnp.where(dx == 2, 12, 10))
        return jnp.where(dy == 0, same, other)

    def b_slot_time(m, q):
        d = (m - z + Z) % Z
        near = jnp.minimum(d, Z - d)
        return jnp.where(near == 0, 0, jnp.where(near == 4, 12 + q % 2, 4 * near - 4 + q))

    def x_step(slot):
        for u, at in enumerate((0, 1, 2, 3, 4, 5, 7, 8, 9, 10, 11, 12)):
            @pl.when(slot == at)
            def _():
                x_copy(True, u, False).wait_recv()
                x_copy(False, u, False).wait_recv()

        for v, at in enumerate((4, 5, 6, 8)):
            @pl.when(slot == at)
            def _():
                y_copy(v, False).wait_recv()

        for u, at in ((2, 0), (3, 1), (4, 2), (5, 3), (6, 4), (7, 5), (8, 6), (9, 8), (10, 9), (11, 10)):
            @pl.when(slot == at)
            def _():
                x_send(jnp.int32(u))

    def slot_body(slot, _):
        z_copy(True, slot, False).wait_recv()
        z_copy(False, slot, False).wait_recv()

        @pl.when(slot < Z_STREAM - 2)
        def _():
            z_send(slot + 2)

        x_step(slot)

        @pl.when(slot == 5)
        def _():
            for d in range(1, 8):
                count_to_row(d).start()

        @pl.when(slot == 8)
        def _():
            for d in range(1, 8):
                count_to_row(d).wait_recv()
            sum_cnt[...] = own_cnt[...] + jnp.sum(row_cnt[...], axis=0)

        @pl.when(slot == 9)
        def _():
            for d in range(1, 8):
                count_to_col(d).start()

        @pl.when(slot == 12)
        def _():
            for d in range(1, 8):
                count_to_col(d).wait_recv()
            everyone = sum_cnt[...] + jnp.sum(col_cnt[...], axis=0)
            tot_out[0] = everyone[0, 0]

        def one_source(m, _):
            a_at = a_slot_time(m)

            def one_piece(q, _):
                @pl.when(jnp.maximum(a_at, b_slot_time(m, q)) == slot)
                def _():
                    multiply(m, q)

                return 0

            @pl.when(a_at <= slot)
            def _():
                lax.fori_loop(0, PIECES, one_piece, 0)

            return 0

        lax.fori_loop(0, Z, one_source, 0)
        return 0

    lax.fori_loop(0, Z_STREAM, slot_body, 0)

    def z_done(t, _):
        z_copy(True, t, True).wait_send()
        z_copy(False, t, True).wait_send()
        return 0

    def x_done(u, _):
        x_copy(True, u, True).wait_send()
        x_copy(False, u, True).wait_send()
        return 0

    def y_done(v, _):
        y_copy(v, True).wait_send()
        return 0

    lax.fori_loop(0, Z_STREAM, z_done, 0)
    lax.fori_loop(0, X_STREAM, x_done, 0)
    lax.fori_loop(0, PIECES, y_done, 0)
    for d in range(1, 8):
        count_to_row(d).wait_send()
        count_to_col(d).wait_send()


def round_kernel(acc, cnt, tot, out, cnt_out, tot_out, stage, sems):
    def piece_out(i):
        rows = pl.ds(i * BLK, BLK)
        return pltpu.make_async_copy(stage.at[:, rows, :], out.at[:, rows, :], sems.at[i])

    for i in range(4):
        rows = slice(i * BLK, (i + 1) * BLK)
        stage[:, rows, :] = acc[:, rows, :].astype(jnp.bfloat16)
        piece_out(i).start()
    for i in range(4):
        for j in range(4):
            cnt_out[i, j] = cnt[i, j]
    tot_out[0] = tot[0]
    for i in range(4):
        piece_out(i).wait()


def shards(a_matrix, b_matrix, a_level, b_level, limit):
    parts, rows, columns = a_matrix.shape
    dma = pltpu.SemaphoreType.DMA
    smem = pl.BlockSpec(memory_space=pltpu.SMEM)
    hbm = pl.BlockSpec(memory_space=pltpu.HBM)
    acc, cnt, tot = pl.pallas_call(
        kernel,
        out_shape=(
            pltpu.VMEM((parts, rows, columns), jnp.float32),
            pltpu.SMEM((4, 4), jnp.int32),
            pltpu.SMEM((1,), jnp.int32),
        ),
        in_specs=[hbm] * 5,
        out_specs=(pl.BlockSpec(memory_space=pltpu.VMEM), smem, smem),
        scratch_shapes=[
            pltpu.SMEM((32, 32), jnp.int32),
            pltpu.SMEM((32, 32), jnp.int32),
            pltpu.SMEM((4, 4), jnp.int32),
            pltpu.VMEM((8, parts, rows, columns), jnp.bfloat16),
            pltpu.VMEM((Z, parts, rows, columns), jnp.bfloat16),
            pltpu.SMEM((32, 16), jnp.float32),
            pltpu.VMEM((8, BLK), jnp.int32),
            pltpu.VMEM((7, 8, BLK), jnp.int32),
            pltpu.VMEM((8, BLK), jnp.int32),
            pltpu.VMEM((7, 8, BLK), jnp.int32),
            dma((3,)),
            dma((2,)),
            dma((Z_STREAM,)), dma((Z_STREAM,)), dma((Z_STREAM,)), dma((Z_STREAM,)),
            dma((X_STREAM,)), dma((X_STREAM,)), dma((X_STREAM,)), dma((X_STREAM,)),
            dma((PIECES,)), dma((PIECES,)),
            dma((7,)), dma((7,)), dma((7,)), dma((7,)),
        ],
        compiler_params=pltpu.CompilerParams(
            collective_id=0, has_side_effects=True, vmem_limit_bytes=61 << 20
        ),
        cost_estimate=pl.CostEstimate(
            flops=8 * rows * 4096 * columns, bytes_accessed=6 << 20, transcendentals=0
        ),
    )(a_level, b_level, limit, a_matrix, b_matrix)
    vmem = pl.BlockSpec(memory_space=pltpu.VMEM)
    return pl.pallas_call(
        round_kernel,
        out_shape=(
            jax.ShapeDtypeStruct((parts, rows, columns), jnp.bfloat16),
            jax.ShapeDtypeStruct((4, 4), jnp.int32),
            jax.ShapeDtypeStruct((1,), jnp.int32),
        ),
        in_specs=[vmem, smem, smem],
        out_specs=(hbm, smem, smem),
        scratch_shapes=[pltpu.VMEM((parts, rows, columns), jnp.bfloat16), dma((4,))],
        compiler_params=pltpu.CompilerParams(vmem_limit_bytes=48 << 20),
    )(acc, cnt, tot)


def solution(mesh):
    placed = (
        P("kpt", "row", "col"),
        P("kpt", "row", "col"),
        P("kpt", None),
        P("kpt", None),
        P(("kpt", "row"), "col"),
    )
    return jax.shard_map(
        shards,
        mesh=mesh,
        in_specs=placed,
        out_specs=(P("kpt", "row", "col"), P(("kpt", "row"), "col"), P("kpt")),
        check_vma=False,
    )
```

```python
import functools

import jax
import jax.numpy as jnp
from jax import lax
from jax.experimental import pallas as pl
from jax.experimental.pallas import tpu as pltpu
from jax.sharding import PartitionSpec as P

BLK = 128
Z = 8
X = 4
PIECES = 4
Z_STREAM = 14
X_STREAM = 12
DEPTH = 4
X_DEPTH = 3
MESH = pl.DeviceIdType.MESH


def piece(ref, slot, q):
    return ref.at[slot, :, pl.ds(pl.multiple_of(q * BLK, BLK), BLK), :]


def kernel(
    a_lev_hbm, b_lev_hbm, lim_hbm, a_hbm, b_hbm,
    acc, cnt_out, tot_out,
    a_lev, b_lev, lim, a_buf, b_buf, scale, power, own_cnt, row_cnt, sum_cnt, col_cnt,
    lev_sem, in_sem, zr_send, zr_recv, zl_send, zl_recv,
    xr_send, xr_recv, xl_send, xl_recv, y_send, y_recv,
    rc_send, rc_recv, cc_send, cc_recv,
    from_right, from_left, from_x_right, from_x_left, from_y, last_in,
):
    z = lax.axis_index("row")
    c = lax.axis_index("col")
    x = c % X
    yh = c // X
    z_right, z_left = (z + 1) % Z, (z + Z - 1) % Z

    def col_at(dx, dy):
        return ((yh + dy) % 2) * X + (x + dx + X) % X

    x_right, x_left, y_far = col_at(1, 0), col_at(-1, 0), col_at(0, 1)

    a_in, b_in = [], []
    for q in range(PIECES):
        rows = pl.ds(q * BLK, BLK)
        b_in.append(
            pltpu.make_async_copy(b_hbm.at[:, rows, :], piece(b_buf, z, q), in_sem.at[q])
        )
        a_in.append(
            pltpu.make_async_copy(a_hbm.at[:, rows, :], piece(a_buf, c, q), in_sem.at[PIECES + q])
        )
        b_in[q].start()
        a_in[q].start()
    levels_in = [
        pltpu.make_async_copy(there, here, lev_sem.at[n])
        for n, (there, here) in enumerate(
            ((a_lev_hbm, a_lev), (b_lev_hbm, b_lev), (lim_hbm, lim))
        )
    ]
    for copy in levels_in:
        copy.start()

    barrier = pltpu.get_barrier_semaphore()

    def signal(sem, **there):
        pl.semaphore_signal(sem, inc=1, device_id=there, device_id_type=MESH)

    def one_if(condition):
        return jnp.where(condition, 1, 0)

    @pl.when(z < Z - 1)
    def _():
        signal(barrier, row=z_right)

    @pl.when(z == 0)
    def _():
        signal(barrier, row=z_left)

    @pl.when(x < X - 1)
    def _():
        signal(barrier, col=x_right)

    @pl.when(x == 0)
    def _():
        signal(barrier, col=x_left)

    @pl.when(yh == 0)
    def _():
        signal(barrier, col=y_far)

    lower = one_if(z > 0) + one_if(z == Z - 1) + one_if(x > 0) + one_if(x == X - 1) + yh

    @pl.when(lower > 0)
    def _():
        pl.semaphore_wait(barrier, lower)


    def z_copy(right, t, sending):
        whole = t < 12
        far = jnp.where(whole, t // PIECES, 3)
        if right:
            q = jnp.where(whole, t % PIECES, t - 12)
            origin = (z - far - (0 if sending else 1) + 2 * Z) % Z
            sems = (zr_send.at[t], zr_recv.at[t])
            there = z_right
        else:
            q = PIECES - 1 - t % PIECES
            origin = (z + far + (0 if sending else 1)) % Z
            sems = (zl_send.at[t], zl_recv.at[t])
            there = z_left
        part = piece(b_buf, origin, q)
        return pltpu.make_async_remote_copy(
            part, part, *sems, device_id={"row": there}, device_id_type=MESH
        )

    def z_last(right, part, sending):
        q = 1 if right or part == 4 else 2
        far = 3 if sending else 4
        origin = (z - far + Z) % Z if right else (z + far) % Z
        sems = (zr_send, zr_recv) if right else (zl_send, zl_recv)
        quarter = 3 if part == 4 else part
        block = b_buf.at[origin, :, pl.ds(q * BLK, BLK), pl.ds(quarter * BLK, BLK)]
        return pltpu.make_async_remote_copy(
            block, block, sems[0].at[Z_STREAM - 1 + part], sems[1].at[Z_STREAM - 1 + part],
            device_id={"row": z_right if right else z_left}, device_id_type=MESH,
        )

    def x_copy(right, u, sending):
        second = u >= 6
        v = jnp.where(second, u - 6, u)
        relayed = v >= 4
        dx = jnp.where(relayed, 1, 0) + (0 if sending else 1)
        dy = jnp.where(second, 1, 0)
        if right:
            q = jnp.where(relayed, v - 4, v)
            sems = (xr_send.at[u], xr_recv.at[u])
            origin, there = col_at(-dx, dy), x_right
        else:
            q = jnp.where(relayed, v - 2, v)
            sems = (xl_send.at[u], xl_recv.at[u])
            origin, there = col_at(dx, dy), x_left
        part = piece(a_buf, origin, q)
        return pltpu.make_async_remote_copy(
            part, part, *sems, device_id={"col": there}, device_id_type=MESH
        )

    def y_copy(v, sending):
        part = piece(a_buf, c if sending else y_far, v)
        return pltpu.make_async_remote_copy(
            part, part, y_send.at[v], y_recv.at[v], device_id={"col": y_far}, device_id_type=MESH
        )

    def count_to_row(d):
        return pltpu.make_async_remote_copy(
            own_cnt, row_cnt.at[d - 1], rc_send.at[d - 1], rc_recv.at[d - 1],
            device_id={"col": (c + d) % 8}, device_id_type=MESH,
        )

    def count_to_col(d):
        return pltpu.make_async_remote_copy(
            sum_cnt, col_cnt.at[d - 1], cc_send.at[d - 1], cc_recv.at[d - 1],
            device_id={"row": (z + d) % Z}, device_id_type=MESH,
        )

    def z_send(t):
        z_copy(True, t, True).start()
        z_copy(False, t, True).start()

    def x_send(u):
        x_copy(True, u, True).start()
        x_copy(False, u, True).start()

    def first_z(right):
        for q in range(DEPTH):
            z_copy(right, jnp.int32(q), True).start()

    def first_x(right):
        for q in range(X_DEPTH):
            x_copy(right, jnp.int32(q), True).start()

    for q in range(DEPTH):
        b_in[q].wait()

    @pl.when(z == Z - 1)
    def _():
        first_z(True)
        signal(from_left, row=z_right)

    @pl.when(z > 0)
    def _():
        first_z(False)
        signal(from_right, row=z_left)

    @pl.when(x == X - 1)
    def _():
        signal(from_x_left, col=x_right)

    @pl.when(x > 0)
    def _():
        signal(from_x_right, col=x_left)

    @pl.when(yh == 1)
    def _():
        signal(from_y, col=y_far)

    @pl.when(z < Z - 1)
    def _():
        pl.semaphore_wait(from_right, 1)
        first_z(True)

    for q in range(PIECES):
        a_in[q].wait()

    @pl.when(x == X - 1)
    def _():
        first_x(True)

    @pl.when(x > 0)
    def _():
        first_x(False)

    @pl.when(yh == 0)
    def _():
        pl.semaphore_wait(from_y, 1)

    for q in range(PIECES):
        y_copy(q, True).start()

    @pl.when(x < X - 1)
    def _():
        pl.semaphore_wait(from_x_right, 1)
        first_x(True)

    @pl.when(x == 0)
    def _():
        pl.semaphore_wait(from_x_left, 1)
        first_x(False)

    @pl.when(z == 0)
    def _():
        pl.semaphore_wait(from_left, 1)
        first_z(False)
        signal(last_in, row=z_right)

    for s in range(33):
        power[s] = 2.0 ** (2 - s) if 2 <= s <= 8 else 0.0

    def tabulate(k, counts):
        new = []
        b_four = []
        for j in range(4):
            b = b_lev[k, 4 * c + j]
            b_four.append(jnp.where(b > 0, b, 16))
        for i in range(4):
            a = a_lev[4 * z + i, k]
            a = jnp.where(a > 0, a, 16)
            for j in range(4):
                both = a + b_four[j]
                keep = both <= lim[i, j]
                scale[k, i * 4 + j] = jnp.where(keep, power[both], 0.0)
                new.append(counts[i * 4 + j] + jnp.where(keep, 1, 0))
        return tuple(new)

    for copy in levels_in:
        copy.wait()
    counts = lax.fori_loop(0, 32, tabulate, (jnp.int32(0),) * 16)
    total = jnp.int32(0)
    for i in range(4):
        for j in range(4):
            cnt_out[i, j] = counts[i * 4 + j]
            total = total + counts[i * 4 + j]
    own_cnt[...] = jnp.full(own_cnt.shape, total, jnp.int32)
    acc[...] = jnp.zeros_like(acc)

    def multiply(m, pieces, columns=range(4)):
        for j in columns:
            cols = pl.ds(j * BLK, BLK)
            lefts, rights = [], []
            for q in pieces:
                lane = pl.ds(pl.multiple_of(q * BLK, BLK), BLK)
                b_re = b_buf[m, 0, lane, cols]
                b_im = b_buf[m, 1, lane, cols]
                rights += [jnp.concatenate([b_re, b_im], 1), jnp.concatenate([-b_im, b_re], 1)]
                bands = []
                for i in range(4):
                    rows = pl.ds(i * BLK, BLK)
                    by = scale[4 * m + q, i * 4 + j].astype(jnp.bfloat16)
                    bands.append(
                        jnp.concatenate([a_buf[m, 0, rows, lane], a_buf[m, 1, rows, lane]], 1) * by
                    )
                lefts.append(jnp.concatenate(bands, 0))
            both = jnp.dot(
                jnp.concatenate(lefts, 1),
                jnp.concatenate(rights, 0),
                preferred_element_type=jnp.float32,
            )
            acc[0, :, cols] += both[:, :BLK]
            acc[1, :, cols] += both[:, BLK:]

    def a_slot_time(m):
        dx = (m % X - x + X) % X
        dy = jnp.where(m // X == yh, 0, 1)
        same = jnp.where(dx == 0, 0, jnp.where(dx == 2, 5, 3))
        other = jnp.where(dx == 0, 8, jnp.where(dx == 2, 12, 10))
        return jnp.where(dy == 0, same, other)

    def b_slot_time(m, q):
        d = (m - z + Z) % Z
        near = jnp.minimum(d, Z - d)
        turn = jnp.where(d < 4, PIECES - 1 - q, q)
        last = jnp.where((q == 1) | (q == 2), Z_STREAM - 1, Z_STREAM - 2)
        return jnp.where(near == 0, 0, jnp.where(near == 4, last, 4 * near - 4 + turn))

    def x_step(slot):
        for u, at in enumerate((0, 1, 2, 3, 4, 5, 7, 8, 9, 10, 11, 12)):
            @pl.when(slot == at)
            def _():
                x_copy(True, u, False).wait_recv()
                x_copy(False, u, False).wait_recv()
                if u > 0:
                    x_copy(True, u - 1, True).wait_send()
                    x_copy(False, u - 1, True).wait_send()

        for v, at in enumerate((4, 5, 6, 8)):
            @pl.when(slot == at)
            def _():
                y_copy(v, False).wait_recv()
                y_copy(v, True).wait_send()

        for u, at in ((3, 0), (4, 2), (5, 3), (6, 4), (7, 5), (8, 6), (9, 8), (10, 9), (11, 10)):
            @pl.when(slot == at)
            def _():
                x_send(jnp.int32(u))

    def slot_body(slot, _):
        z_copy(True, slot, False).wait_recv()
        z_copy(False, slot, False).wait_recv()

        @pl.when(slot == 9)
        def _():
            for d in range(1, 8):
                count_to_col(d).start()

        @pl.when(slot < Z_STREAM - 1 - DEPTH)
        def _():
            z_send(slot + DEPTH)

        @pl.when(slot == Z_STREAM - 1 - DEPTH)
        def _():
            for part in range(3):
                z_last(True, part, True).start()
                z_last(False, part, True).start()

            z_last(False, 3, True).start()

            @pl.when(z < Z - 1)
            def _():
                z_last(True, 3, True).start()

        @pl.when((slot == 10) & (z == 1))
        def _():
            z_last(False, 4, True).start()

        for place in (1, 2, 3):

            @pl.when((slot == 5 + place) & (z == place))
            def _():
                pl.semaphore_wait(last_in, 1)
                if place < 3:
                    signal(last_in, row=z_right)

        @pl.when(slot >= 2)
        def _():
            z_copy(True, slot - 2, True).wait_send()
            z_copy(False, slot - 2, True).wait_send()

        x_step(slot)

        @pl.when(slot == 5)
        def _():
            for d in range(1, 8):
                count_to_row(d).start()

        @pl.when(slot == 8)
        def _():
            for d in range(1, 8):
                count_to_row(d).wait_recv()
                count_to_row(d).wait_send()
            sum_cnt[...] = own_cnt[...] + jnp.sum(row_cnt[...], axis=0)

        def one_source(m, _):
            a_at = a_slot_time(m)

            def one_piece(q, _):
                @pl.when(jnp.maximum(a_at, b_slot_time(m, q)) == slot)
                def _():
                    multiply(m, (q,))

                return 0

            @pl.when(a_at <= slot)
            def _():
                lax.fori_loop(0, PIECES, one_piece, 0)

            return 0

        lax.fori_loop(0, Z, one_source, 0)
        return 0

    lax.fori_loop(0, Z_STREAM - 1, slot_body, 0)

    for d in range(1, 8):
        count_to_col(d).wait_recv()
        count_to_col(d).wait_send()
    everyone = sum_cnt[...] + jnp.sum(col_cnt[...], axis=0)
    tot_out[0] = everyone[0, 0]

    across = (z + 4) % Z
    for part in range(4):
        if part < 3:
            z_last(True, part, False).wait_recv()
        else:

            @pl.when(z > 0)
            def _():
                z_last(True, 3, False).wait_recv()

            @pl.when(z == 0)
            def _():
                z_last(False, 4, False).wait_recv()

        z_last(False, part, False).wait_recv()
    multiply(across, (1, 2))

    for right in (True, False):
        for t in (Z_STREAM - 3, Z_STREAM - 2):
            z_copy(right, t, True).wait_send()
        for part in range(3):
            z_last(right, part, True).wait_send()
        x_copy(right, X_STREAM - 1, True).wait_send()
    z_last(False, 3, True).wait_send()

    @pl.when(z < Z - 1)
    def _():
        z_last(True, 3, True).wait_send()

    @pl.when(z == 1)
    def _():
        z_last(False, 4, True).wait_send()


def round_kernel(acc, cnt, tot, out, cnt_out, tot_out, stage, sems):
    copies = [
        pltpu.make_async_copy(cnt, cnt_out, sems.at[4]),
        pltpu.make_async_copy(tot, tot_out, sems.at[5]),
    ]
    for copy in copies:
        copy.start()
    for i in range(4):
        rows = pl.ds(i * BLK, BLK)
        stage[:, i * BLK : (i + 1) * BLK, :] = acc[:, i * BLK : (i + 1) * BLK, :].astype(
            jnp.bfloat16
        )
        copy = pltpu.make_async_copy(stage.at[:, rows, :], out.at[:, rows, :], sems.at[i])
        copy.start()
        copies.append(copy)
    for copy in copies:
        copy.wait()


def shards(a_matrix, b_matrix, a_level, b_level, limit):
    parts, rows, columns = a_matrix.shape
    dma = pltpu.SemaphoreType.DMA
    smem = pl.BlockSpec(memory_space=pltpu.SMEM)
    hbm = pl.BlockSpec(memory_space=pltpu.HBM)
    acc, cnt, tot = pl.pallas_call(
        kernel,
        out_shape=(
            pltpu.VMEM((parts, rows, columns), jnp.float32),
            pltpu.SMEM((4, 4), jnp.int32),
            pltpu.SMEM((1,), jnp.int32),
        ),
        in_specs=[hbm] * 5,
        out_specs=(pl.BlockSpec(memory_space=pltpu.VMEM), smem, smem),
        scratch_shapes=[
            pltpu.SMEM((32, 32), jnp.int32),
            pltpu.SMEM((32, 32), jnp.int32),
            pltpu.SMEM((4, 4), jnp.int32),
            pltpu.VMEM((8, parts, rows, columns), jnp.bfloat16),
            pltpu.VMEM((Z, parts, rows, columns), jnp.bfloat16),
            pltpu.SMEM((32, 16), jnp.float32),
            pltpu.SMEM((33,), jnp.float32),
            pltpu.VMEM((1, BLK), jnp.int32),
            pltpu.VMEM((7, 1, BLK), jnp.int32),
            pltpu.VMEM((1, BLK), jnp.int32),
            pltpu.VMEM((7, 1, BLK), jnp.int32),
            dma((3,)),
            dma((2 * PIECES,)),
            dma((Z_STREAM + 4,)), dma((Z_STREAM + 4,)), dma((Z_STREAM + 4,)), dma((Z_STREAM + 4,)),
            dma((X_STREAM,)), dma((X_STREAM,)), dma((X_STREAM,)), dma((X_STREAM,)),
            dma((PIECES,)), dma((PIECES,)),
            dma((7,)), dma((7,)), dma((7,)), dma((7,)),
        ] + [pltpu.SemaphoreType.REGULAR] * 6,
        compiler_params=pltpu.CompilerParams(
            collective_id=0, has_side_effects=True, vmem_limit_bytes=61 << 20
        ),
        cost_estimate=pl.CostEstimate(
            flops=8 * rows * 4096 * columns, bytes_accessed=6 << 20, transcendentals=0
        ),
    )(a_level, b_level, limit, a_matrix, b_matrix)
    vmem = pl.BlockSpec(memory_space=pltpu.VMEM)
    return pl.pallas_call(
        round_kernel,
        out_shape=(
            jax.ShapeDtypeStruct((parts, rows, columns), jnp.bfloat16),
            jax.ShapeDtypeStruct((4, 4), jnp.int32),
            jax.ShapeDtypeStruct((1,), jnp.int32),
        ),
        in_specs=[vmem, smem, smem],
        out_specs=(hbm, hbm, hbm),
        scratch_shapes=[pltpu.VMEM((parts, rows, columns), jnp.bfloat16), dma((6,))],
        compiler_params=pltpu.CompilerParams(vmem_limit_bytes=48 << 20),
    )(acc, cnt, tot)


def solution(mesh):
    placed = (
        P("kpt", "row", "col"),
        P("kpt", "row", "col"),
        P("kpt", None),
        P("kpt", None),
        P(("kpt", "row"), "col"),
    )
    return jax.shard_map(
        shards,
        mesh=mesh,
        in_specs=placed,
        out_specs=(P("kpt", "row", "col"), P(("kpt", "row"), "col"), P("kpt")),
        check_vma=False,
    )
```

```python
import functools

import jax
import jax.numpy as jnp
from jax import lax
from jax.experimental import pallas as pl
from jax.experimental.pallas import tpu as pltpu
from jax.sharding import PartitionSpec as P

BLK = 128
Z = 8
X = 4
PIECES = 4
Z_STREAM = 14
X_STREAM = 12
DEPTH = 4
X_DEPTH = 3
SHIFT = 48
MESH = pl.DeviceIdType.MESH


def piece(ref, slot, q):
    return ref.at[slot, :, pl.ds(pl.multiple_of(q * BLK, BLK), BLK), :]


def kernel(
    a_lev_hbm, b_lev_hbm, lim_hbm, a_hbm, b_hbm,
    acc, cnt_out, tot_out,
    a_lev, b_lev, lim, a_buf, b_buf, scale, power, own_cnt, row_cnt, sum_cnt, col_cnt,
    lev_sem, in_sem, zr_send, zr_recv, zl_send, zl_recv,
    xr_send, xr_recv, xl_send, xl_recv, y_send, y_recv,
    rc_send, rc_recv, cc_send, cc_recv,
    from_right, from_left, from_x_right, from_x_left, from_y, last_in,
):
    z = lax.axis_index("row")
    c = lax.axis_index("col")
    x = c % X
    yh = c // X
    z_right, z_left = (z + 1) % Z, (z + Z - 1) % Z

    def col_at(dx, dy):
        return ((yh + dy) % 2) * X + (x + dx + X) % X

    x_right, x_left, y_far = col_at(1, 0), col_at(-1, 0), col_at(0, 1)

    a_in, b_in = [], []
    for q in range(PIECES):
        rows = pl.ds(q * BLK, BLK)
        b_in.append(
            pltpu.make_async_copy(b_hbm.at[:, rows, :], piece(b_buf, z, q), in_sem.at[q])
        )
        a_in.append(
            pltpu.make_async_copy(a_hbm.at[:, rows, :], piece(a_buf, c, q), in_sem.at[PIECES + q])
        )
    for q in (0, 3, 1, 2):
        b_in[q].start()
    for q in range(PIECES):
        a_in[q].start()
    levels_in = [
        pltpu.make_async_copy(there, here, lev_sem.at[n])
        for n, (there, here) in enumerate(
            ((a_lev_hbm, a_lev), (b_lev_hbm, b_lev), (lim_hbm, lim))
        )
    ]
    for copy in levels_in:
        copy.start()

    barrier = pltpu.get_barrier_semaphore()

    def signal(sem, **there):
        pl.semaphore_signal(sem, inc=1, device_id=there, device_id_type=MESH)

    def one_if(condition):
        return jnp.where(condition, 1, 0)

    @pl.when(z < Z - 1)
    def _():
        signal(barrier, row=z_right)

    @pl.when(z == 0)
    def _():
        signal(barrier, row=z_left)

    @pl.when(x < X - 1)
    def _():
        signal(barrier, col=x_right)

    @pl.when(x == 0)
    def _():
        signal(barrier, col=x_left)

    @pl.when(yh == 0)
    def _():
        signal(barrier, col=y_far)

    lower = one_if(z > 0) + one_if(z == Z - 1) + one_if(x > 0) + one_if(x == X - 1) + yh

    @pl.when(lower > 0)
    def _():
        pl.semaphore_wait(barrier, lower)


    def z_copy(right, t, sending):
        whole = t < 12
        far = jnp.where(whole, t // PIECES, 3)
        if right:
            q = jnp.where(whole, t % PIECES, t - 12)
            origin = (z - far - (0 if sending else 1) + 2 * Z) % Z
            sems = (zr_send.at[t], zr_recv.at[t])
            there = z_right
        else:
            q = PIECES - 1 - t % PIECES
            origin = (z + far + (0 if sending else 1)) % Z
            sems = (zl_send.at[t], zl_recv.at[t])
            there = z_left
        part = piece(b_buf, origin, q)
        return pltpu.make_async_remote_copy(
            part, part, *sems, device_id={"row": there}, device_id_type=MESH
        )

    def z_last(right, part, sending):
        q = 1 if right or part == 1 else 2
        far = 3 if sending else 4
        origin = (z - far + Z) % Z if right else (z + far) % Z
        sems = (zr_send, zr_recv) if right else (zl_send, zl_recv)
        begin = BLK - SHIFT if part == 1 else 0
        end = BLK - SHIFT if right and part == 0 else BLK
        rows = b_buf.at[origin, :, pl.ds(q * BLK + begin, end - begin), :]
        return pltpu.make_async_remote_copy(
            rows, rows, sems[0].at[Z_STREAM - 1 + part], sems[1].at[Z_STREAM - 1 + part],
            device_id={"row": z_right if right else z_left}, device_id_type=MESH,
        )

    def x_copy(right, u, sending):
        second = u >= 6
        v = jnp.where(second, u - 6, u)
        relayed = v >= 4
        dx = jnp.where(relayed, 1, 0) + (0 if sending else 1)
        dy = jnp.where(second, 1, 0)
        if right:
            q = jnp.where(relayed, v - 4, v)
            sems = (xr_send.at[u], xr_recv.at[u])
            origin, there = col_at(-dx, dy), x_right
        else:
            q = jnp.where(relayed, v - 2, v)
            sems = (xl_send.at[u], xl_recv.at[u])
            origin, there = col_at(dx, dy), x_left
        part = piece(a_buf, origin, q)
        return pltpu.make_async_remote_copy(
            part, part, *sems, device_id={"col": there}, device_id_type=MESH
        )

    def y_copy(v, sending):
        part = piece(a_buf, c if sending else y_far, v)
        return pltpu.make_async_remote_copy(
            part, part, y_send.at[v], y_recv.at[v], device_id={"col": y_far}, device_id_type=MESH
        )

    def count_to_row(d):
        return pltpu.make_async_remote_copy(
            own_cnt, row_cnt.at[d - 1], rc_send.at[d - 1], rc_recv.at[d - 1],
            device_id={"col": (c + d) % 8}, device_id_type=MESH,
        )

    def count_to_col(d):
        return pltpu.make_async_remote_copy(
            sum_cnt, col_cnt.at[d - 1], cc_send.at[d - 1], cc_recv.at[d - 1],
            device_id={"row": (z + d) % Z}, device_id_type=MESH,
        )

    def z_send(t):
        z_copy(True, t, True).start()
        z_copy(False, t, True).start()

    def x_send(u):
        x_copy(True, u, True).start()
        x_copy(False, u, True).start()

    def first_z(right):
        for q in range(DEPTH):
            z_copy(right, jnp.int32(q), True).start()

    def first_x(right):
        for q in range(X_DEPTH):
            x_copy(right, jnp.int32(q), True).start()

    @pl.when(z == Z - 1)
    def _():
        signal(from_left, row=z_right)

    @pl.when(z > 0)
    def _():
        signal(from_right, row=z_left)

    @pl.when(x == X - 1)
    def _():
        signal(from_x_left, col=x_right)

    @pl.when(x > 0)
    def _():
        signal(from_x_right, col=x_left)

    @pl.when(yh == 1)
    def _():
        signal(from_y, col=y_far)

    for q, to_right, to_left in ((0, (0,), ()), (3, (), (0,)), (1, (1,), ()), (2, (2, 3), (1, 2, 3))):
        b_in[q].wait()
        if to_right:

            @pl.when(z == Z - 1)
            def _():
                for t in to_right:
                    z_copy(True, jnp.int32(t), True).start()

        if to_left:

            @pl.when(z > 0)
            def _():
                for t in to_left:
                    z_copy(False, jnp.int32(t), True).start()

    @pl.when(z < Z - 1)
    def _():
        pl.semaphore_wait(from_right, 1)
        first_z(True)

    for q in range(PIECES):
        a_in[q].wait()

    @pl.when(x == X - 1)
    def _():
        first_x(True)

    @pl.when(x > 0)
    def _():
        first_x(False)

    @pl.when(yh == 0)
    def _():
        pl.semaphore_wait(from_y, 1)

    for q in range(PIECES):
        y_copy(q, True).start()

    @pl.when(x < X - 1)
    def _():
        pl.semaphore_wait(from_x_right, 1)
        first_x(True)

    @pl.when(x == 0)
    def _():
        pl.semaphore_wait(from_x_left, 1)
        first_x(False)

    @pl.when(z == 0)
    def _():
        pl.semaphore_wait(from_left, 1)
        first_z(False)
        signal(last_in, row=z_right)

    for s in range(33):
        power[s] = 2.0 ** (2 - s) if 2 <= s <= 8 else 0.0

    def tabulate(k, counts):
        new = []
        b_four = []
        for j in range(4):
            b = b_lev[k, 4 * c + j]
            b_four.append(jnp.where(b > 0, b, 16))
        for i in range(4):
            a = a_lev[4 * z + i, k]
            a = jnp.where(a > 0, a, 16)
            for j in range(4):
                both = a + b_four[j]
                keep = both <= lim[i, j]
                scale[k, i * 4 + j] = jnp.where(keep, power[both], 0.0)
                new.append(counts[i * 4 + j] + jnp.where(keep, 1, 0))
        return tuple(new)

    for copy in levels_in:
        copy.wait()
    counts = lax.fori_loop(0, 32, tabulate, (jnp.int32(0),) * 16)
    total = jnp.int32(0)
    for i in range(4):
        for j in range(4):
            cnt_out[i, j] = counts[i * 4 + j]
            total = total + counts[i * 4 + j]
    own_cnt[...] = jnp.full(own_cnt.shape, total, jnp.int32)
    acc[...] = jnp.zeros_like(acc)

    def multiply(m, pieces, columns=range(4)):
        for j in columns:
            cols = pl.ds(j * BLK, BLK)
            lefts, rights = [], []
            for q in pieces:
                lane = pl.ds(pl.multiple_of(q * BLK, BLK), BLK)
                b_re = b_buf[m, 0, lane, cols]
                b_im = b_buf[m, 1, lane, cols]
                rights += [jnp.concatenate([b_re, b_im], 1), jnp.concatenate([-b_im, b_re], 1)]
                bands = []
                for i in range(4):
                    rows = pl.ds(i * BLK, BLK)
                    by = scale[4 * m + q, i * 4 + j].astype(jnp.bfloat16)
                    bands.append(
                        jnp.concatenate([a_buf[m, 0, rows, lane], a_buf[m, 1, rows, lane]], 1) * by
                    )
                lefts.append(jnp.concatenate(bands, 0))
            both = jnp.dot(
                jnp.concatenate(lefts, 1),
                jnp.concatenate(rights, 0),
                preferred_element_type=jnp.float32,
            )
            acc[0, :, cols] += both[:, :BLK]
            acc[1, :, cols] += both[:, BLK:]

    def a_slot_time(m):
        dx = (m % X - x + X) % X
        dy = jnp.where(m // X == yh, 0, 1)
        same = jnp.where(dx == 0, 0, jnp.where(dx == 2, 5, 3))
        other = jnp.where(dx == 0, 8, jnp.where(dx == 2, 12, 10))
        return jnp.where(dy == 0, same, other)

    def b_slot_time(m, q):
        d = (m - z + Z) % Z
        near = jnp.minimum(d, Z - d)
        turn = jnp.where(d < 4, PIECES - 1 - q, q)
        last = jnp.where((q == 1) | (q == 2), Z_STREAM - 1, Z_STREAM - 2)
        return jnp.where(near == 0, 0, jnp.where(near == 4, last, 4 * near - 4 + turn))

    def x_step(slot):
        for u, at in enumerate((0, 1, 2, 3, 4, 5, 7, 8, 9, 10, 11, 12)):
            @pl.when(slot == at)
            def _():
                x_copy(True, u, False).wait_recv()
                x_copy(False, u, False).wait_recv()
                if u > 0:
                    x_copy(True, u - 1, True).wait_send()
                    x_copy(False, u - 1, True).wait_send()

        for v, at in enumerate((4, 5, 6, 8)):
            @pl.when(slot == at)
            def _():
                y_copy(v, False).wait_recv()
                y_copy(v, True).wait_send()

        for u, at in ((3, 0), (4, 2), (5, 3), (6, 4), (7, 5), (8, 6), (9, 8), (10, 9), (11, 10)):
            @pl.when(slot == at)
            def _():
                x_send(jnp.int32(u))

    def slot_body(slot, _):
        z_copy(True, slot, False).wait_recv()
        z_copy(False, slot, False).wait_recv()

        @pl.when(slot == 9)
        def _():
            for d in range(1, 8):
                count_to_col(d).start()

        @pl.when(slot < Z_STREAM - 1 - DEPTH)
        def _():
            z_send(slot + DEPTH)

        @pl.when(slot == Z_STREAM - 1 - DEPTH)
        def _():
            z_last(True, 0, True).start()
            z_last(False, 0, True).start()

            @pl.when(z < Z - 1)
            def _():
                z_last(True, 1, True).start()

        @pl.when((slot == 10) & (z == 1))
        def _():
            z_last(False, 1, True).start()

        for place in (1, 2, 3):

            @pl.when((slot == 5 + place) & (z == place))
            def _():
                pl.semaphore_wait(last_in, 1)
                if place < 3:
                    signal(last_in, row=z_right)

        @pl.when(slot >= 2)
        def _():
            z_copy(True, slot - 2, True).wait_send()
            z_copy(False, slot - 2, True).wait_send()

        x_step(slot)

        @pl.when(slot == 5)
        def _():
            for d in range(1, 8):
                count_to_row(d).start()

        @pl.when(slot == 8)
        def _():
            for d in range(1, 8):
                count_to_row(d).wait_recv()
                count_to_row(d).wait_send()
            sum_cnt[...] = own_cnt[...] + jnp.sum(row_cnt[...], axis=0)

        def one_source(m, _):
            a_at = a_slot_time(m)

            def one_piece(q, _):
                @pl.when(jnp.maximum(a_at, b_slot_time(m, q)) == slot)
                def _():
                    multiply(m, (q,))

                return 0

            @pl.when(a_at <= slot)
            def _():
                lax.fori_loop(0, PIECES, one_piece, 0)

            return 0

        lax.fori_loop(0, Z, one_source, 0)
        return 0

    lax.fori_loop(0, Z_STREAM - 1, slot_body, 0)

    for d in range(1, 8):
        count_to_col(d).wait_recv()
        count_to_col(d).wait_send()
    everyone = sum_cnt[...] + jnp.sum(col_cnt[...], axis=0)
    tot_out[0] = everyone[0, 0]

    across = (z + 4) % Z
    z_last(True, 0, False).wait_recv()
    z_last(False, 0, False).wait_recv()

    @pl.when(z > 0)
    def _():
        z_last(True, 1, False).wait_recv()

    @pl.when(z == 0)
    def _():
        z_last(False, 1, False).wait_recv()

    multiply(across, (1, 2))

    for right in (True, False):
        for t in (Z_STREAM - 3, Z_STREAM - 2):
            z_copy(right, t, True).wait_send()
        z_last(right, 0, True).wait_send()
        x_copy(right, X_STREAM - 1, True).wait_send()

    @pl.when(z < Z - 1)
    def _():
        z_last(True, 1, True).wait_send()

    @pl.when(z == 1)
    def _():
        z_last(False, 1, True).wait_send()


def round_kernel(acc, cnt, tot, out, cnt_out, tot_out, stage, sems):
    copies = [
        pltpu.make_async_copy(cnt, cnt_out, sems.at[4]),
        pltpu.make_async_copy(tot, tot_out, sems.at[5]),
    ]
    for copy in copies:
        copy.start()
    for i in range(4):
        rows = pl.ds(i * BLK, BLK)
        stage[:, i * BLK : (i + 1) * BLK, :] = acc[:, i * BLK : (i + 1) * BLK, :].astype(
            jnp.bfloat16
        )
        copy = pltpu.make_async_copy(stage.at[:, rows, :], out.at[:, rows, :], sems.at[i])
        copy.start()
        copies.append(copy)
    for copy in copies:
        copy.wait()


def shards(a_matrix, b_matrix, a_level, b_level, limit):
    parts, rows, columns = a_matrix.shape
    dma = pltpu.SemaphoreType.DMA
    smem = pl.BlockSpec(memory_space=pltpu.SMEM)
    hbm = pl.BlockSpec(memory_space=pltpu.HBM)
    acc, cnt, tot = pl.pallas_call(
        kernel,
        out_shape=(
            pltpu.VMEM((parts, rows, columns), jnp.float32),
            pltpu.SMEM((4, 4), jnp.int32),
            pltpu.SMEM((1,), jnp.int32),
        ),
        in_specs=[hbm] * 5,
        out_specs=(pl.BlockSpec(memory_space=pltpu.VMEM), smem, smem),
        scratch_shapes=[
            pltpu.SMEM((32, 32), jnp.int32),
            pltpu.SMEM((32, 32), jnp.int32),
            pltpu.SMEM((4, 4), jnp.int32),
            pltpu.VMEM((8, parts, rows, columns), jnp.bfloat16),
            pltpu.VMEM((Z, parts, rows, columns), jnp.bfloat16),
            pltpu.SMEM((32, 16), jnp.float32),
            pltpu.SMEM((33,), jnp.float32),
            pltpu.VMEM((1, BLK), jnp.int32),
            pltpu.VMEM((7, 1, BLK), jnp.int32),
            pltpu.VMEM((1, BLK), jnp.int32),
            pltpu.VMEM((7, 1, BLK), jnp.int32),
            dma((3,)),
            dma((2 * PIECES,)),
            dma((Z_STREAM + 1,)), dma((Z_STREAM + 1,)), dma((Z_STREAM + 1,)), dma((Z_STREAM + 1,)),
            dma((X_STREAM,)), dma((X_STREAM,)), dma((X_STREAM,)), dma((X_STREAM,)),
            dma((PIECES,)), dma((PIECES,)),
            dma((7,)), dma((7,)), dma((7,)), dma((7,)),
        ] + [pltpu.SemaphoreType.REGULAR] * 6,
        compiler_params=pltpu.CompilerParams(
            collective_id=0, has_side_effects=True, vmem_limit_bytes=61 << 20
        ),
        cost_estimate=pl.CostEstimate(
            flops=8 * rows * 4096 * columns, bytes_accessed=6 << 20, transcendentals=0
        ),
    )(a_level, b_level, limit, a_matrix, b_matrix)
    vmem = pl.BlockSpec(memory_space=pltpu.VMEM)
    return pl.pallas_call(
        round_kernel,
        out_shape=(
            jax.ShapeDtypeStruct((parts, rows, columns), jnp.bfloat16),
            jax.ShapeDtypeStruct((4, 4), jnp.int32),
            jax.ShapeDtypeStruct((1,), jnp.int32),
        ),
        in_specs=[vmem, smem, smem],
        out_specs=(hbm, hbm, hbm),
        scratch_shapes=[pltpu.VMEM((parts, rows, columns), jnp.bfloat16), dma((6,))],
        compiler_params=pltpu.CompilerParams(vmem_limit_bytes=48 << 20),
    )(acc, cnt, tot)


def solution(mesh):
    placed = (
        P("kpt", "row", "col"),
        P("kpt", "row", "col"),
        P("kpt", None),
        P("kpt", None),
        P(("kpt", "row"), "col"),
    )
    return jax.shard_map(
        shards,
        mesh=mesh,
        in_specs=placed,
        out_specs=(P("kpt", "row", "col"), P(("kpt", "row"), "col"), P("kpt")),
        check_vma=False,
    )
```

```python
import functools

import jax
import jax.numpy as jnp
from jax import lax
from jax.experimental import pallas as pl
from jax.experimental.pallas import tpu as pltpu
from jax.sharding import PartitionSpec as P

BLK = 128
Z = 8
X = 4
PIECES = 4
Z_STREAM = 14
X_STREAM = 12
DEPTH = 4
X_DEPTH = 3
SHIFT = 48
MESH = pl.DeviceIdType.MESH


def piece(ref, slot, q):
    return ref.at[slot, :, pl.ds(pl.multiple_of(q * BLK, BLK), BLK), :]


def kernel(
    a_lev_hbm, b_lev_hbm, lim_hbm, a_hbm, b_hbm,
    acc, cnt_out, tot_out,
    a_lev, b_lev, lim, a_buf, b_buf, scale, power, own_cnt, row_cnt, sum_cnt, col_cnt,
    lev_sem, in_sem, zr_send, zr_recv, zl_send, zl_recv,
    xr_send, xr_recv, xl_send, xl_recv, y_send, y_recv,
    rc_send, rc_recv, cc_send, cc_recv,
    from_right, from_left, from_x_right, from_x_left, from_y, last_in,
):
    z = lax.axis_index("row")
    c = lax.axis_index("col")
    x = c % X
    yh = c // X
    z_right, z_left = (z + 1) % Z, (z + Z - 1) % Z

    def col_at(dx, dy):
        return ((yh + dy) % 2) * X + (x + dx + X) % X

    x_right, x_left, y_far = col_at(1, 0), col_at(-1, 0), col_at(0, 1)

    a_in, b_in = [], []
    for q in range(PIECES):
        rows = pl.ds(q * BLK, BLK)
        b_in.append(
            pltpu.make_async_copy(b_hbm.at[:, rows, :], piece(b_buf, z, q), in_sem.at[q])
        )
        a_in.append(
            pltpu.make_async_copy(a_hbm.at[:, rows, :], piece(a_buf, c, q), in_sem.at[PIECES + q])
        )
    for q in (0, 3, 1, 2):
        b_in[q].start()
    for q in range(PIECES):
        a_in[q].start()
    levels_in = [
        pltpu.make_async_copy(there, here, lev_sem.at[n])
        for n, (there, here) in enumerate(
            ((a_lev_hbm, a_lev), (b_lev_hbm, b_lev), (lim_hbm, lim))
        )
    ]
    for copy in levels_in:
        copy.start()

    barrier = pltpu.get_barrier_semaphore()

    def signal(sem, **there):
        pl.semaphore_signal(sem, inc=1, device_id=there, device_id_type=MESH)

    def one_if(condition):
        return jnp.where(condition, 1, 0)

    @pl.when(z < Z - 1)
    def _():
        signal(barrier, row=z_right)

    @pl.when(z == 0)
    def _():
        signal(barrier, row=z_left)

    @pl.when(x < X - 1)
    def _():
        signal(barrier, col=x_right)

    @pl.when(x == 0)
    def _():
        signal(barrier, col=x_left)

    @pl.when(yh == 0)
    def _():
        signal(barrier, col=y_far)

    lower = one_if(z > 0) + one_if(z == Z - 1) + one_if(x > 0) + one_if(x == X - 1) + yh

    @pl.when(lower > 0)
    def _():
        pl.semaphore_wait(barrier, lower)


    def z_copy(right, t, sending):
        whole = t < 12
        far = jnp.where(whole, t // PIECES, 3)
        if right:
            q = jnp.where(whole, t % PIECES, t - 12)
            origin = (z - far - (0 if sending else 1) + 2 * Z) % Z
            sems = (zr_send.at[t], zr_recv.at[t])
            there = z_right
        else:
            q = PIECES - 1 - t % PIECES
            origin = (z + far + (0 if sending else 1)) % Z
            sems = (zl_send.at[t], zl_recv.at[t])
            there = z_left
        part = piece(b_buf, origin, q)
        return pltpu.make_async_remote_copy(
            part, part, *sems, device_id={"row": there}, device_id_type=MESH
        )

    def z_last(right, part, sending):
        q = 1 if right or part == 1 else 2
        far = 3 if sending else 4
        origin = (z - far + Z) % Z if right else (z + far) % Z
        sems = (zr_send, zr_recv) if right else (zl_send, zl_recv)
        begin = BLK - SHIFT if part == 1 else 0
        end = BLK - SHIFT if right and part == 0 else BLK
        rows = b_buf.at[origin, :, pl.ds(q * BLK + begin, end - begin), :]
        return pltpu.make_async_remote_copy(
            rows, rows, sems[0].at[Z_STREAM - 1 + part], sems[1].at[Z_STREAM - 1 + part],
            device_id={"row": z_right if right else z_left}, device_id_type=MESH,
        )

    def x_copy(right, u, sending):
        second = u >= 6
        v = jnp.where(second, u - 6, u)
        relayed = v >= 4
        dx = jnp.where(relayed, 1, 0) + (0 if sending else 1)
        dy = jnp.where(second, 1, 0)
        if right:
            q = jnp.where(relayed, v - 4, v)
            sems = (xr_send.at[u], xr_recv.at[u])
            origin, there = col_at(-dx, dy), x_right
        else:
            q = jnp.where(relayed, v - 2, v)
            sems = (xl_send.at[u], xl_recv.at[u])
            origin, there = col_at(dx, dy), x_left
        part = piece(a_buf, origin, q)
        return pltpu.make_async_remote_copy(
            part, part, *sems, device_id={"col": there}, device_id_type=MESH
        )

    def y_copy(v, sending):
        part = piece(a_buf, c if sending else y_far, v)
        return pltpu.make_async_remote_copy(
            part, part, y_send.at[v], y_recv.at[v], device_id={"col": y_far}, device_id_type=MESH
        )

    def count_to_row(d):
        return pltpu.make_async_remote_copy(
            own_cnt, row_cnt.at[d - 1], rc_send.at[d - 1], rc_recv.at[d - 1],
            device_id={"col": (c + d) % 8}, device_id_type=MESH,
        )

    def count_to_col(d):
        return pltpu.make_async_remote_copy(
            sum_cnt, col_cnt.at[d - 1], cc_send.at[d - 1], cc_recv.at[d - 1],
            device_id={"row": (z + d) % Z}, device_id_type=MESH,
        )

    def z_send(t):
        z_copy(True, t, True).start()
        z_copy(False, t, True).start()

    def x_send(u):
        x_copy(True, u, True).start()
        x_copy(False, u, True).start()

    def first_z(right):
        for q in range(DEPTH):
            z_copy(right, jnp.int32(q), True).start()

    def first_x(right):
        for q in range(X_DEPTH):
            x_copy(right, jnp.int32(q), True).start()

    @pl.when(z == Z - 1)
    def _():
        signal(from_left, row=z_right)

    @pl.when(z > 0)
    def _():
        signal(from_right, row=z_left)

    @pl.when(x == X - 1)
    def _():
        signal(from_x_left, col=x_right)

    @pl.when(x > 0)
    def _():
        signal(from_x_right, col=x_left)

    @pl.when(yh == 1)
    def _():
        signal(from_y, col=y_far)

    for q, to_right, to_left in ((0, (0,), ()), (3, (), (0,)), (1, (1,), ()), (2, (2, 3), (1, 2, 3))):
        b_in[q].wait()
        if to_right:

            @pl.when(z == Z - 1)
            def _():
                for t in to_right:
                    z_copy(True, jnp.int32(t), True).start()

        if to_left:

            @pl.when(z > 0)
            def _():
                for t in to_left:
                    z_copy(False, jnp.int32(t), True).start()

    @pl.when(z < Z - 1)
    def _():
        pl.semaphore_wait(from_right, 1)
        first_z(True)

    for q in range(PIECES):
        a_in[q].wait()

    @pl.when(x == X - 1)
    def _():
        first_x(True)

    @pl.when(x > 0)
    def _():
        first_x(False)

    @pl.when(yh == 0)
    def _():
        pl.semaphore_wait(from_y, 1)

    for q in range(PIECES):
        y_copy(q, True).start()

    @pl.when(x < X - 1)
    def _():
        pl.semaphore_wait(from_x_right, 1)
        first_x(True)

    @pl.when(x == 0)
    def _():
        pl.semaphore_wait(from_x_left, 1)
        first_x(False)

    @pl.when(z == 0)
    def _():
        pl.semaphore_wait(from_left, 1)
        first_z(False)
        signal(last_in, row=z_right)

    for s in range(33):
        power[s] = 2.0 ** (2 - s) if 2 <= s <= 8 else 0.0

    def tabulate(k, counts):
        new = []
        b_four = []
        for j in range(4):
            b = b_lev[k, 4 * c + j]
            b_four.append(jnp.where(b > 0, b, 16))
        for i in range(4):
            a = a_lev[4 * z + i, k]
            a = jnp.where(a > 0, a, 16)
            for j in range(4):
                both = a + b_four[j]
                keep = both <= lim[i, j]
                scale[k, i * 4 + j] = jnp.where(keep, power[both], 0.0)
                new.append(counts[i * 4 + j] + jnp.where(keep, 1, 0))
        return tuple(new)

    for copy in levels_in:
        copy.wait()
    counts = lax.fori_loop(0, 32, tabulate, (jnp.int32(0),) * 16)
    total = jnp.int32(0)
    for i in range(4):
        for j in range(4):
            cnt_out[i, j] = counts[i * 4 + j]
            total = total + counts[i * 4 + j]
    own_cnt[...] = jnp.full(own_cnt.shape, total, jnp.int32)
    acc[...] = jnp.zeros_like(acc)

    def multiply(m, pieces, columns=range(4)):
        for j in columns:
            cols = pl.ds(j * BLK, BLK)
            lefts, rights = [], []
            for q in pieces:
                lane = pl.ds(pl.multiple_of(q * BLK, BLK), BLK)
                b_re = b_buf[m, 0, lane, cols]
                b_im = b_buf[m, 1, lane, cols]
                rights += [jnp.concatenate([b_re, b_im], 1), jnp.concatenate([-b_im, b_re], 1)]
                bands = []
                for i in range(4):
                    rows = pl.ds(i * BLK, BLK)
                    by = scale[4 * m + q, i * 4 + j].astype(jnp.bfloat16)
                    bands.append(
                        jnp.concatenate([a_buf[m, 0, rows, lane], a_buf[m, 1, rows, lane]], 1) * by
                    )
                lefts.append(jnp.concatenate(bands, 0))
            both = jnp.dot(
                jnp.concatenate(lefts, 1),
                jnp.concatenate(rights, 0),
                preferred_element_type=jnp.float32,
            )
            acc[0, :, cols] += both[:, :BLK]
            acc[1, :, cols] += both[:, BLK:]

    def a_slot_time(m):
        dx = (m % X - x + X) % X
        dy = jnp.where(m // X == yh, 0, 1)
        same = jnp.where(dx == 0, 0, jnp.where(dx == 2, 5, 3))
        other = jnp.where(dx == 0, 8, jnp.where(dx == 2, 12, 10))
        return jnp.where(dy == 0, same, other)

    def b_slot_time(m, q):
        d = (m - z + Z) % Z
        near = jnp.minimum(d, Z - d)
        turn = jnp.where(d < 4, PIECES - 1 - q, q)
        last = jnp.where((q == 1) | (q == 2), Z_STREAM - 1, Z_STREAM - 2)
        return jnp.where(near == 0, 0, jnp.where(near == 4, last, 4 * near - 4 + turn))

    def x_step(slot):
        for u, at in enumerate((0, 1, 2, 3, 4, 5, 7, 8, 9, 10, 11, 12)):
            @pl.when(slot == at)
            def _():
                x_copy(True, u, False).wait_recv()
                x_copy(False, u, False).wait_recv()
                if u > 0:
                    x_copy(True, u - 1, True).wait_send()
                    x_copy(False, u - 1, True).wait_send()

        for v, at in enumerate((4, 5, 6, 8)):
            @pl.when(slot == at)
            def _():
                y_copy(v, False).wait_recv()
                y_copy(v, True).wait_send()

        for u, at in ((3, 0), (4, 2), (5, 3), (6, 4), (7, 5), (8, 6), (9, 8), (10, 9), (11, 10)):
            @pl.when(slot == at)
            def _():
                x_send(jnp.int32(u))

    def slot_body(slot, _):
        z_copy(True, slot, False).wait_recv()
        z_copy(False, slot, False).wait_recv()

        @pl.when(slot == 9)
        def _():
            for d in range(1, 8):
                count_to_col(d).start()

        @pl.when(slot < Z_STREAM - 1 - DEPTH)
        def _():
            z_send(slot + DEPTH)

        @pl.when(slot == Z_STREAM - 1 - DEPTH)
        def _():
            z_last(True, 0, True).start()
            z_last(False, 0, True).start()

            @pl.when(z < Z - 1)
            def _():
                z_last(True, 1, True).start()

        @pl.when((slot == 10) & (z == 1))
        def _():
            z_last(False, 1, True).start()

        for place in (1, 2, 3):

            @pl.when((slot == 5 + place) & (z == place))
            def _():
                pl.semaphore_wait(last_in, 1)
                if place < 3:
                    signal(last_in, row=z_right)

        @pl.when(slot >= 2)
        def _():
            z_copy(True, slot - 2, True).wait_send()
            z_copy(False, slot - 2, True).wait_send()

        x_step(slot)

        @pl.when(slot == 5)
        def _():
            for d in range(1, 8):
                count_to_row(d).start()

        @pl.when(slot == 8)
        def _():
            for d in range(1, 8):
                count_to_row(d).wait_recv()
                count_to_row(d).wait_send()
            sum_cnt[...] = own_cnt[...] + jnp.sum(row_cnt[...], axis=0)

        def one_source(m, _):
            a_at = a_slot_time(m)

            def one_piece(q, _):
                @pl.when(jnp.maximum(a_at, b_slot_time(m, q)) == slot)
                def _():
                    multiply(m, (q,))

                return 0

            @pl.when(a_at <= slot)
            def _():
                lax.fori_loop(0, PIECES, one_piece, 0)

            return 0

        lax.fori_loop(0, Z, one_source, 0)
        return 0

    lax.fori_loop(0, Z_STREAM - 1, slot_body, 0)

    for d in range(1, 8):
        count_to_col(d).wait_recv()
        count_to_col(d).wait_send()
    everyone = sum_cnt[...] + jnp.sum(col_cnt[...], axis=0)
    tot_out[0] = everyone[0, 0]

    across = (z + 4) % Z
    z_last(True, 0, False).wait_recv()
    z_last(False, 0, False).wait_recv()

    @pl.when(z > 0)
    def _():
        z_last(True, 1, False).wait_recv()

    @pl.when(z == 0)
    def _():
        z_last(False, 1, False).wait_recv()

    multiply(across, (1, 2))

    for right in (True, False):
        for t in (Z_STREAM - 3, Z_STREAM - 2):
            z_copy(right, t, True).wait_send()
        z_last(right, 0, True).wait_send()
        x_copy(right, X_STREAM - 1, True).wait_send()

    @pl.when(z < Z - 1)
    def _():
        z_last(True, 1, True).wait_send()

    @pl.when(z == 1)
    def _():
        z_last(False, 1, True).wait_send()


def round_kernel(acc, cnt, tot, out, cnt_out, tot_out, stage, sems):
    copies = [
        pltpu.make_async_copy(cnt, cnt_out, sems.at[8]),
        pltpu.make_async_copy(tot, tot_out, sems.at[9]),
    ]
    for copy in copies:
        copy.start()
    half = BLK // 2
    for i in range(8):
        rows = pl.ds(i * half, half)
        stage[:, i * half : (i + 1) * half, :] = acc[:, i * half : (i + 1) * half, :].astype(
            jnp.bfloat16
        )
        copy = pltpu.make_async_copy(stage.at[:, rows, :], out.at[:, rows, :], sems.at[i])
        copy.start()
        copies.append(copy)
    for copy in copies:
        copy.wait()


def shards(a_matrix, b_matrix, a_level, b_level, limit):
    parts, rows, columns = a_matrix.shape
    dma = pltpu.SemaphoreType.DMA
    smem = pl.BlockSpec(memory_space=pltpu.SMEM)
    hbm = pl.BlockSpec(memory_space=pltpu.HBM)
    acc, cnt, tot = pl.pallas_call(
        kernel,
        out_shape=(
            pltpu.VMEM((parts, rows, columns), jnp.float32),
            pltpu.SMEM((4, 4), jnp.int32),
            pltpu.SMEM((1,), jnp.int32),
        ),
        in_specs=[hbm] * 5,
        out_specs=(pl.BlockSpec(memory_space=pltpu.VMEM), smem, smem),
        scratch_shapes=[
            pltpu.SMEM((32, 32), jnp.int32),
            pltpu.SMEM((32, 32), jnp.int32),
            pltpu.SMEM((4, 4), jnp.int32),
            pltpu.VMEM((8, parts, rows, columns), jnp.bfloat16),
            pltpu.VMEM((Z, parts, rows, columns), jnp.bfloat16),
            pltpu.SMEM((32, 16), jnp.float32),
            pltpu.SMEM((33,), jnp.float32),
            pltpu.VMEM((1, BLK), jnp.int32),
            pltpu.VMEM((7, 1, BLK), jnp.int32),
            pltpu.VMEM((1, BLK), jnp.int32),
            pltpu.VMEM((7, 1, BLK), jnp.int32),
            dma((3,)),
            dma((2 * PIECES,)),
            dma((Z_STREAM + 1,)), dma((Z_STREAM + 1,)), dma((Z_STREAM + 1,)), dma((Z_STREAM + 1,)),
            dma((X_STREAM,)), dma((X_STREAM,)), dma((X_STREAM,)), dma((X_STREAM,)),
            dma((PIECES,)), dma((PIECES,)),
            dma((7,)), dma((7,)), dma((7,)), dma((7,)),
        ] + [pltpu.SemaphoreType.REGULAR] * 6,
        compiler_params=pltpu.CompilerParams(
            collective_id=0, has_side_effects=True, vmem_limit_bytes=61 << 20
        ),
        cost_estimate=pl.CostEstimate(
            flops=8 * rows * 4096 * columns, bytes_accessed=6 << 20, transcendentals=0
        ),
    )(a_level, b_level, limit, a_matrix, b_matrix)
    vmem = pl.BlockSpec(memory_space=pltpu.VMEM)
    return pl.pallas_call(
        round_kernel,
        out_shape=(
            jax.ShapeDtypeStruct((parts, rows, columns), jnp.bfloat16),
            jax.ShapeDtypeStruct((4, 4), jnp.int32),
            jax.ShapeDtypeStruct((1,), jnp.int32),
        ),
        in_specs=[vmem, smem, smem],
        out_specs=(hbm, hbm, hbm),
        scratch_shapes=[pltpu.VMEM((parts, rows, columns), jnp.bfloat16), dma((10,))],
        compiler_params=pltpu.CompilerParams(vmem_limit_bytes=48 << 20),
    )(acc, cnt, tot)


def solution(mesh):
    placed = (
        P("kpt", "row", "col"),
        P("kpt", "row", "col"),
        P("kpt", None),
        P("kpt", None),
        P(("kpt", "row"), "col"),
    )
    return jax.shard_map(
        shards,
        mesh=mesh,
        in_specs=placed,
        out_specs=(P("kpt", "row", "col"), P(("kpt", "row"), "col"), P("kpt")),
        check_vma=False,
    )
```
